32 devices in a mesh: g: 32 (over z, y, x, core).
Axes of the slice: x: 2, y: 2, z: 4, core: 2. Of those that a mesh axis runs over, the one named last changes fastest.
Arguments:
- node_feat: bfloat16 [16384, 8448], P(None, 'g')
- w_self1: bfloat16 [8448, 256], P('g')
- w_nbr1: bfloat16 [8448, 256], P('g')
- nbr_ids: int32 [16384, 15], P('g')
- nbr_mask: int32 [16384, 15], P('g')
- w_self2: bfloat16 [256, 256], replicated
- w_nbr2: bfloat16 [256, 256], replicated
- w_self3: bfloat16 [256, 5], replicated
- w_nbr3: bfloat16 [256, 5], replicated
Outputs:
- output: float32 [16384, 5], P('g')
All inputs are finite; a program needn't handle non-finite values.
Results may differ from the reference program's by a relative error of at most 0.00945678.
Values are sent between devices in bfloat16 or wider.
A program may use at most 1 GiB of HBM per device.

```python
import jax
import jax.numpy as jnp
from jax import lax

FEAT_DIM = 8448
HIDDEN = 256
CLASSES = 5
FAN_IN = 15
NUM_NODES = 16384
HOT_NODES = NUM_NODES // 16


def draw_graph(graph_key):
    key_ids, key_hot, key_pick, key_deg = jax.random.split(graph_key, 4)
    wide_ids = jax.random.randint(key_ids, (NUM_NODES, FAN_IN), 0, NUM_NODES)
    hot_ids = jax.random.randint(key_hot, (NUM_NODES, FAN_IN), 0, HOT_NODES)
    pick_hot = jax.random.randint(key_pick, (NUM_NODES, FAN_IN), 0, 4) == 0
    nbr_ids = jnp.where(pick_hot, hot_ids, wide_ids)
    nbr_ids = nbr_ids.at[0, 0].set(NUM_NODES - 1).at[NUM_NODES - 1, 0].set(0).astype(jnp.int32)
    degree = jax.random.randint(key_deg, (NUM_NODES,), 1, FAN_IN + 1)
    degree = degree.at[0].set(FAN_IN).at[1].set(1)
    nbr_mask = (jnp.arange(FAN_IN)[None, :] < degree[:, None]).astype(jnp.int32)
    return nbr_ids, nbr_mask


def dense_weight(weight_key, fan_rows, fan_cols):
    normal_draw = jax.random.normal(weight_key, (fan_rows, fan_cols), jnp.float32)
    return (normal_draw * fan_rows ** -0.5).astype(jnp.bfloat16)


def setup_inputs(seed: int = 0) -> dict:
    key_list = jax.random.split(jax.random.key(seed), 8)
    nbr_ids, nbr_mask = draw_graph(key_list[0])
    node_feat = jax.random.normal(key_list[1], (NUM_NODES, FEAT_DIM), jnp.float32).astype(jnp.bfloat16)
    return {
        "node_feat": node_feat,
        "w_self1": dense_weight(key_list[2], FEAT_DIM, HIDDEN),
        "w_nbr1": dense_weight(key_list[3], FEAT_DIM, HIDDEN),
        "nbr_ids": nbr_ids,
        "nbr_mask": nbr_mask,
        "w_self2": dense_weight(key_list[4], HIDDEN, HIDDEN),
        "w_nbr2": dense_weight(key_list[5], HIDDEN, HIDDEN),
        "w_self3": dense_weight(key_list[6], HIDDEN, CLASSES),
        "w_nbr3": dense_weight(key_list[7], HIDDEN, CLASSES),
    }


def nbr_mean(row_data, nbr_ids, nbr_mask):
    mask_f = nbr_mask.astype(jnp.float32)

    def add_slot(acc_sum, slot_cols):
        ids_col, mask_col = slot_cols
        return acc_sum + mask_col[:, None] * row_data[ids_col].astype(jnp.float32), None

    zero_acc = jnp.zeros((nbr_ids.shape[0], row_data.shape[1]), jnp.float32)
    slot_sum, _ = lax.scan(add_slot, zero_acc, (nbr_ids.T, mask_f.T))
    return slot_sum / jnp.sum(mask_f, axis=1, keepdims=True)


def reference(node_feat, w_self1, w_nbr1, nbr_ids, nbr_mask, w_self2, w_nbr2, w_self3, w_nbr3):
    self_part = jnp.dot(node_feat, w_self1, preferred_element_type=jnp.float32)
    nbr_proj = jnp.dot(node_feat, w_nbr1, preferred_element_type=jnp.float32)
    hidden1 = jax.nn.relu(self_part + nbr_mean(nbr_proj, nbr_ids, nbr_mask)).astype(jnp.bfloat16)
    mean_one = nbr_mean(hidden1, nbr_ids, nbr_mask).astype(jnp.bfloat16)
    pre_two = jnp.dot(hidden1, w_self2, preferred_element_type=jnp.float32) + jnp.dot(mean_one, w_nbr2, preferred_element_type=jnp.float32)
    hidden2 = jax.nn.relu(pre_two).astype(jnp.bfloat16)
    mean_two = nbr_mean(hidden2, nbr_ids, nbr_mask).astype(jnp.bfloat16)
    logits = jnp.dot(hidden2, w_self3, preferred_element_type=jnp.float32) + jnp.dot(mean_two, w_nbr3, preferred_element_type=jnp.float32)
    return logits
```

```python
import functools

import jax
import jax.numpy as jnp
from jax import lax
from jax.experimental import pallas as pl
from jax.experimental.pallas import tpu as pltpu
from jax.sharding import PartitionSpec as P

MESH = pl.DeviceIdType.MESH
BF = jnp.bfloat16
F32 = jnp.float32


def place():
    me = lax.axis_index("g")
    core = lax.rem(me, 2)
    x = lax.rem(me // 2, 2)
    y = lax.rem(me // 4, 2)
    z = me // 8
    return me, me + 1 - 2 * core, me + 2 - 4 * x, me + 4 - 8 * y, z


def along_z(dev, z, j):
    return dev + 8 * (lax.rem(z + j, 4) - z)


def greet(peers):
    barrier = pltpu.get_barrier_semaphore()
    for peer in peers:
        pl.semaphore_signal(barrier, inc=1, device_id=(peer,), device_id_type=MESH)
    pl.semaphore_wait(barrier, len(peers))


def remote(src, dst, send_sem, recv_sem, dev):
    return pltpu.make_async_remote_copy(
        src_ref=src, dst_ref=dst, send_sem=send_sem, recv_sem=recv_sem, device_id=(dev,), device_id_type=MESH
    )


STEPS = (2, 1, 3, 0)
DG, XN, YN, ME = range(4)


def scatter_kernel(
    feat, w_ref, nbr_out, self_out,
    own, got, w_got, to_x, to_y, from_x, from_y, to_z, from_z,
    own_sem, gs_sem, gr_sem, w_sem, xs_sem, xr_sem, ys_sem, yr_sem, zs_sem, zr_sem,
):
    me, mate, xn, yn, z = place()
    dg = xn + yn - me
    hid, rows = nbr_out.shape
    greet([mate, xn, yn] + [along_z(me, z, j) for j in (1, 2, 3)])
    mate_shift = mate - me

    w_copy = remote(w_ref, w_got, w_sem.at[0], w_sem.at[1], mate)
    w_copy.start()
    own_copies, mate_copies = [], []
    for t, j in enumerate(STEPS):
        for q, dev in ((DG, dg), (XN, xn), (YN, yn), (ME, me)):
            slot = t * 4 + q
            dest = along_z(dev, z, j)
            a = pltpu.make_async_copy(feat.at[:, pl.ds(pl.multiple_of(dest * rows, rows), rows)], own.at[slot], own_sem.at[slot])
            a.start()
            b = remote(
                feat.at[:, pl.ds(pl.multiple_of((dest + mate_shift) * rows, rows), rows)], got.at[slot],
                gs_sem.at[slot], gr_sem.at[slot], mate,
            )
            b.start()
            own_copies.append(a)
            mate_copies.append(b)

    chunk = 256

    def project(slot, half, r):
        part = pl.ds(half * hid, hid)
        return jnp.dot(w_ref[part, :], own[slot, :, pl.ds(r, chunk)], preferred_element_type=F32) + jnp.dot(
            w_got[part, :], got[slot, :, pl.ds(r, chunk)], preferred_element_type=F32
        )

    def tiles(body):
        def step(i, carry):
            body(pl.multiple_of(i * chunk, chunk))
            return carry

        lax.fori_loop(0, rows // chunk, step, 0)

    def ready(slot):
        own_copies[slot].wait()
        mate_copies[slot].wait_recv()

    copies = {}

    def send_x(t, m):
        c = remote(to_x.at[t, m], from_x.at[t, m], xs_sem.at[t, m], xr_sem.at[t, m], xn)
        c.start()
        copies["x", t, m] = c

    def send_y(t, m):
        c = remote(to_y.at[t, m], from_y.at[t, m], ys_sem.at[t, m], yr_sem.at[t, m], yn)
        c.start()
        copies["y", t, m] = c

    def stage_one(t):
        ready(t * 4 + DG)

        def body(r):
            to_x[t, 0, :, pl.ds(r, chunk)] = project(t * 4 + DG, 0, r).astype(BF)
            to_y[t, 0, :, pl.ds(r, chunk)] = project(t * 4 + DG, 1, r).astype(BF)

        tiles(body)
        send_x(t, 0)
        send_y(t, 0)
        ready(t * 4 + XN)
        ready(t * 4 + YN)

        def body_raw(r):
            to_x[t, 1, :, pl.ds(r, chunk)] = project(t * 4 + XN, 0, r).astype(BF)
            to_y[t, 1, :, pl.ds(r, chunk)] = project(t * 4 + YN, 1, r).astype(BF)

        tiles(body_raw)
        send_x(t, 1)
        send_y(t, 1)

    def stage_relay(t):
        copies["x", t, 0].wait_recv()
        copies["y", t, 0].wait_recv()

        def body(r):
            to_x[t, 2, :, pl.ds(r, chunk)] = (project(t * 4 + XN, 1, r) + from_y[t, 0, :, pl.ds(r, chunk)].astype(F32)).astype(BF)
            to_y[t, 2, :, pl.ds(r, chunk)] = (project(t * 4 + YN, 0, r) + from_x[t, 0, :, pl.ds(r, chunk)].astype(F32)).astype(BF)

        tiles(body)
        send_x(t, 2)
        send_y(t, 2)

    def plane_sum(t, half, r):
        mx, my = (1, 2) if half == 0 else (2, 1)
        return (
            project(t * 4 + ME, half, r)
            + from_x[t, mx, :, pl.ds(r, chunk)].astype(F32)
            + from_y[t, my, :, pl.ds(r, chunk)].astype(F32)
        )

    def plane_ready(t):
        ready(t * 4 + ME)
        for m in (1, 2):
            copies["x", t, m].wait_recv()
            copies["y", t, m].wait_recv()

    def stage_z(t):
        plane_ready(t)
        j = STEPS[t]

        def body(r):
            for half in (0, 1):
                to_z[t, half, :, pl.ds(r, chunk)] = plane_sum(t, half, r).astype(BF)

        tiles(body)
        c = remote(to_z.at[t], from_z.at[3 - j], zs_sem.at[t], zr_sem.at[3 - j], along_z(me, z, j))
        c.start()
        copies["z", t] = c

    w_copy.wait_recv()
    stage_one(0)
    stage_one(1)
    stage_relay(0)
    stage_one(2)
    stage_relay(1)
    stage_z(0)
    stage_one(3)
    stage_relay(2)
    stage_z(1)
    stage_relay(3)
    stage_z(2)
    plane_ready(3)
    for k in range(3):
        remote(to_z.at[k], from_z.at[k], zs_sem.at[k], zr_sem.at[k], me).wait_recv()

    def last(r):
        at = pl.ds(r, chunk)
        total = [
            plane_sum(3, half, r) + from_z[0, half, :, at].astype(F32) + from_z[1, half, :, at].astype(F32) + from_z[2, half, :, at].astype(F32)
            for half in (0, 1)
        ]
        nbr_out[:, at] = total[0].astype(BF)
        self_out[:, at] = total[1]

    tiles(last)
    w_copy.wait_send()
    for c in mate_copies:
        c.wait_send()
    for c in copies.values():
        c.wait_send()


def scatter(feat, weights, rows):
    both, depth = weights.shape
    hid = both // 2
    vmem = pl.BlockSpec(memory_space=pltpu.VMEM)
    dma = pltpu.SemaphoreType.DMA
    return pl.pallas_call(
        scatter_kernel,
        out_shape=(jax.ShapeDtypeStruct((hid, rows), BF), jax.ShapeDtypeStruct((hid, rows), F32)),
        in_specs=[pl.BlockSpec(memory_space=pl.ANY), vmem],
        out_specs=(vmem, vmem),
        scratch_shapes=[
            pltpu.VMEM((16, depth, rows), BF),
            pltpu.VMEM((16, depth, rows), BF),
            pltpu.VMEM((both, depth), BF),
            pltpu.VMEM((4, 3, hid, rows), BF),
            pltpu.VMEM((4, 3, hid, rows), BF),
            pltpu.VMEM((4, 3, hid, rows), BF),
            pltpu.VMEM((4, 3, hid, rows), BF),
            pltpu.VMEM((3, 2, hid, rows), BF),
            pltpu.VMEM((3, 2, hid, rows), BF),
            dma((16,)), dma((16,)), dma((16,)), dma((2,)),
            dma((4, 3)), dma((4, 3)), dma((4, 3)), dma((4, 3)), dma((3,)), dma((3,)),
        ],
        compiler_params=pltpu.CompilerParams(collective_id=0, has_side_effects=True),
        name="scatter",
    )(feat, weights)


def count_kernel(ids, out):
    fan = ids.shape[0]
    tall, wide = out.shape
    base = pl.program_id(0) * tall
    step = 32

    def body(t, carry):
        r = pl.multiple_of(t * step, step)
        node = lax.broadcasted_iota(jnp.int32, (step, wide), 0) + (base + r)
        total = jnp.zeros((step, wide), F32)
        for k in range(fan):
            total = jnp.where(ids[pl.ds(k, 1), :] == node, total + 1.0, total)
        out[pl.ds(r, step), :] = total.astype(BF)
        return carry

    lax.fori_loop(0, tall // step, body, 0)


def count(ids, n):
    fan, rows = ids.shape
    return pl.pallas_call(
        count_kernel,
        grid=(n,),
        out_shape=jax.ShapeDtypeStruct((n, rows, rows), BF),
        in_specs=[pl.BlockSpec((fan, rows), lambda b: (0, 0))],
        out_specs=pl.BlockSpec((None, rows, rows), lambda b: (b, 0, 0)),
        name="count",
    )(ids)


def gather_kernel(layer, *refs):
    counts, mask, rows_in = refs[:3]
    extra = refs[3:4] if layer == 1 else refs[3:5]
    (out, full, edges, total, ed_sem, xs_sem, xr_sem, ys_sem, yr_sem, zs_sem, zr_sem, cs_sem, cr_sem) = refs[3 + len(extra):]
    me, mate, xn, yn, z = place()
    dg = xn + yn - me
    hid, rows = rows_in.shape
    half = hid // 2
    greet([mate, xn, yn] + [along_z(me, z, j) for j in (1, 2, 3)])
    top, bottom = pl.ds(0, half), pl.ds(half, half)
    started = []

    def go(src, dst, send_sem, recv_sem, dev):
        c = remote(src, dst, send_sem, recv_sem, dev)
        c.start()
        started.append(c)

    def arrived(dst, recv_sem, send_sem):
        remote(dst, dst, send_sem, recv_sem, me).wait_recv()

    for j in (1, 3, 2):
        go(rows_in, full.at[me], zs_sem.at[j - 1], zr_sem.at[3 - j], along_z(me, z, j))
    go(rows_in, full.at[me], xs_sem.at[0], xr_sem.at[0], xn)
    go(rows_in, full.at[me], ys_sem.at[0], yr_sem.at[0], yn)
    go(rows_in, full.at[me], cs_sem.at[0], cr_sem.at[0], mate)
    loads = [pltpu.make_async_copy(counts.at[pl.ds(8 * q, 8)], edges.at[pl.ds(8 * q, 8)], ed_sem.at[q]) for q in range(4)]
    for load in loads:
        load.start()
    for load in loads:
        load.wait()

    chunk = 256

    def add(src, b, first=False):
        def body(i, carry):
            at = pl.ds(pl.multiple_of(i * chunk, chunk), chunk)
            part = jnp.dot(src[...], edges[b, :, at], preferred_element_type=F32)
            total[:, at] = part if first else total[:, at] + part
            return carry

        lax.fori_loop(0, rows // chunk, body, 0)

    add(rows_in, me, True)

    def column(j):
        b = along_z(me, z, j)
        arrived(full.at[b], zr_sem.at[j - 1], zs_sem.at[j - 1])
        go(full.at[b], full.at[b], xs_sem.at[j], xr_sem.at[j], xn)
        go(full.at[b], full.at[b], ys_sem.at[j], yr_sem.at[j], yn)
        go(full.at[b], full.at[b], cs_sem.at[j], cr_sem.at[j], mate)
        add(full.at[b], b)

    def relay(j):
        bx, by = along_z(xn, z, j), along_z(yn, z, j)
        arrived(full.at[bx], xr_sem.at[j], xs_sem.at[j])
        go(full.at[bx, top], full.at[bx, top], ys_sem.at[4 + j], yr_sem.at[4 + j], yn)
        go(full.at[bx], full.at[bx], cs_sem.at[4 + j], cr_sem.at[4 + j], mate)
        arrived(full.at[by], yr_sem.at[j], ys_sem.at[j])
        go(full.at[by, bottom], full.at[by, bottom], xs_sem.at[4 + j], xr_sem.at[4 + j], xn)
        go(full.at[by], full.at[by], cs_sem.at[8 + j], cr_sem.at[8 + j], mate)
        add(full.at[bx], bx)
        add(full.at[by], by)

    def diagonal(j):
        b = along_z(dg, z, j)
        arrived(full.at[b, top], yr_sem.at[4 + j], ys_sem.at[4 + j])
        go(full.at[b, top], full.at[b, top], cs_sem.at[12 + j], cr_sem.at[12 + j], mate)
        arrived(full.at[b, bottom], xr_sem.at[4 + j], xs_sem.at[4 + j])
        go(full.at[b, bottom], full.at[b, bottom], cs_sem.at[16 + j], cr_sem.at[16 + j], mate)
        add(full.at[b], b)

    shift = mate - me

    def from_mate(j):
        for k, dev in ((0, me), (4, xn), (8, yn)):
            b = along_z(dev, z, j) + shift
            arrived(full.at[b], cr_sem.at[k + j], cs_sem.at[k + j])
            add(full.at[b], b)

    def from_mate_diagonal(j):
        b = along_z(dg, z, j) + shift
        arrived(full.at[b, top], cr_sem.at[12 + j], cs_sem.at[12 + j])
        arrived(full.at[b, bottom], cr_sem.at[16 + j], cs_sem.at[16 + j])
        add(full.at[b], b)

    column(1)
    column(3)
    relay(0)
    column(2)
    relay(1)
    relay(3)
    diagonal(0)
    relay(2)
    from_mate(0)
    from_mate(1)
    from_mate(3)
    diagonal(1)
    from_mate_diagonal(0)
    diagonal(3)
    from_mate(2)
    from_mate_diagonal(1)
    from_mate_diagonal(3)
    diagonal(2)
    from_mate_diagonal(2)

    mean = total[...] * (1.0 / jnp.sum(mask[...].astype(F32), axis=0, keepdims=True))
    if layer == 1:
        out[...] = jnp.maximum(extra[0][...] + mean, 0.0).astype(BF)
    else:
        w_self, w_nbr = extra
        pre = jnp.dot(w_self[...], rows_in[...], preferred_element_type=F32) + jnp.dot(
            w_nbr[...], mean.astype(BF), preferred_element_type=F32
        )
        out[...] = jnp.maximum(pre, 0.0).astype(BF) if layer == 2 else pre
    for c in started:
        c.wait_send()


def gather(layer, counts, mask, rows_in, *extra):
    hid, rows = rows_in.shape
    n = counts.shape[0]
    vmem = pl.BlockSpec(memory_space=pltpu.VMEM)
    dma = pltpu.SemaphoreType.DMA
    cols = extra[-1].shape[0]
    return pl.pallas_call(
        functools.partial(gather_kernel, layer),
        out_shape=jax.ShapeDtypeStruct((cols, rows), F32 if layer == 3 else BF),
        in_specs=[pl.BlockSpec(memory_space=pl.ANY)] + [vmem] * (2 + len(extra)),
        out_specs=vmem,
        scratch_shapes=[
            pltpu.VMEM((n, hid, rows), BF),
            pltpu.VMEM((n, rows, rows), BF),
            pltpu.VMEM((hid, rows), F32),
            dma((4,)), dma((8,)), dma((8,)), dma((8,)), dma((8,)), dma((3,)), dma((3,)), dma((20,)), dma((20,)),
        ],
        compiler_params=pltpu.CompilerParams(collective_id=layer, has_side_effects=True),
        name=f"gather{layer}",
    )(counts, mask, rows_in, *extra)


def solution(mesh):
    def device_step(feat, w_self1, w_nbr1, ids, mask, w_self2, w_nbr2, w_self3, w_nbr3):
        rows = ids.shape[0]
        mask = mask.T
        listed = jnp.where(mask > 0, ids.T, -1)
        counts = count(listed, feat.shape[0] // rows)
        nbr1, self1 = scatter(feat.T, jnp.concatenate([w_nbr1.T, w_self1.T], axis=0), rows)
        hidden1 = gather(1, counts, mask, nbr1, self1)
        hidden2 = gather(2, counts, mask, hidden1, w_self2.T, w_nbr2.T)
        return gather(3, counts, mask, hidden2, w_self3.T, w_nbr3.T).T

    col_split, row_split, replicated = P(None, "g"), P("g", None), P()
    return jax.shard_map(
        device_step,
        mesh=mesh,
        in_specs=(col_split, row_split, row_split, row_split, row_split, replicated, replicated, replicated, replicated),
        out_specs=row_split,
        check_vma=False,
    )
```

```python
import jax
import jax.numpy as jnp
from jax import lax
from jax.experimental import pallas as pl
from jax.experimental.pallas import tpu as pltpu
from jax.sharding import PartitionSpec as P

MESH = pl.DeviceIdType.MESH
BF = jnp.bfloat16
F32 = jnp.float32
DG, XN, YN, ME = range(4)


def remote(src, dst, send_sem, recv_sem, dev):
    return pltpu.make_async_remote_copy(
        src_ref=src, dst_ref=dst, send_sem=send_sem, recv_sem=recv_sem, device_id=(dev,), device_id_type=MESH
    )


def kernel(
    feat, w_ref, ids, mask, w_self2, w_nbr2, w_self3, w_nbr3, out,
    own, got, w_got, to_x, to_y, from_x, from_y, to_z, from_z, listed, edges, full, total, self1, hidden,
    own_sem, gs_sem, gr_sem, w_sem, sxs_sem, sxr_sem, sys_sem, syr_sem, szs_sem, szr_sem,
    xs_sem, xr_sem, ys_sem, yr_sem, zs_sem, zr_sem, cs_sem, cr_sem,
):
    me = lax.axis_index("g")
    core = lax.rem(me, 2)
    x = lax.rem(me // 2, 2)
    y = lax.rem(me // 4, 2)
    z = me // 8
    mate, xn, yn = me + 1 - 2 * core, me + 2 - 4 * x, me + 4 - 8 * y
    dg = xn + yn - me
    f = (z * (3 - z)) // 2
    inner = f == 1
    across, beyond = 3 - z, z + 2 - 4 * (z // 2)
    planes = (z, z + 1 - 2 * lax.rem(z, 2), f * across + (1 - f) * beyond, f * beyond + (1 - f) * across)

    def at_plane(dev, k):
        return dev + 8 * (planes[k] - z)

    pair = at_plane(me, 1)
    facing = me + 8 * (across - z)
    hid, rows = self1.shape
    half = hid // 2
    chunk = 256

    barrier = pltpu.get_barrier_semaphore()
    for peer in (mate, xn, yn, pair, facing):
        pl.semaphore_signal(barrier, inc=1, device_id=(peer,), device_id_type=MESH)
    pl.semaphore_wait(barrier, 5)

    def tiles(body):
        def step(i, carry):
            body(pl.ds(pl.multiple_of(i * chunk, chunk), chunk))
            return carry

        lax.fori_loop(0, rows // chunk, step, 0)


    w_copy = remote(w_ref, w_got, w_sem.at[0], w_sem.at[1], mate)
    w_copy.start()
    own_copies, mate_copies = {}, {}
    mate_shift = mate - me

    def fetch(t):
        for q, dev in ((DG, dg), (XN, xn), (YN, yn), (ME, me)):
            slot = t * 4 + q
            dest = at_plane(dev, 3 - t)
            a = pltpu.make_async_copy(
                feat.at[:, pl.ds(pl.multiple_of(dest * rows, rows), rows)], own.at[slot], own_sem.at[slot]
            )
            a.start()
            b = remote(
                feat.at[:, pl.ds(pl.multiple_of((dest + mate_shift) * rows, rows), rows)],
                got.at[slot], gs_sem.at[slot], gr_sem.at[slot], mate,
            )
            b.start()
            own_copies[slot], mate_copies[slot] = a, b

    def ready(slot):
        own_copies[slot].wait()
        mate_copies[slot].wait_recv()

    def project(slot, part, at):
        of = pl.ds(part * hid, hid)
        return jnp.dot(w_ref[of, :], own[slot, :, at], preferred_element_type=F32) + jnp.dot(
            w_got[of, :], got[slot, :, at], preferred_element_type=F32
        )

    copies = {}

    def send_plane(t, m):
        for name, src, dst, ss, rs, dev in (
            ("x", to_x, from_x, sxs_sem, sxr_sem, xn), ("y", to_y, from_y, sys_sem, syr_sem, yn),
        ):
            c = remote(src.at[t, m], dst.at[t, m], ss.at[t, m], rs.at[t, m], dev)
            c.start()
            copies[name, t, m] = c

    def received(t, m):
        copies["x", t, m].wait_recv()
        copies["y", t, m].wait_recv()

    def diagonal_out(t):
        ready(t * 4 + DG)

        def body(at):
            to_x[t, 0, :, at] = project(t * 4 + DG, 0, at).astype(BF)
            to_y[t, 0, :, at] = project(t * 4 + DG, 1, at).astype(BF)

        tiles(body)
        send_plane(t, 0)

    def raw_out(t):
        ready(t * 4 + XN)
        ready(t * 4 + YN)

        def body(at):
            to_x[t, 1, :, at] = project(t * 4 + XN, 0, at).astype(BF)
            to_y[t, 1, :, at] = project(t * 4 + YN, 1, at).astype(BF)

        tiles(body)
        send_plane(t, 1)

    def relay_out(t):
        received(t, 0)

        def body(at):
            to_x[t, 2, :, at] = (project(t * 4 + XN, 1, at) + from_y[t, 0, :, at].astype(F32)).astype(BF)
            to_y[t, 2, :, at] = (project(t * 4 + YN, 0, at) + from_x[t, 0, :, at].astype(F32)).astype(BF)

        tiles(body)
        send_plane(t, 2)

    def plane_sum(t, part, at):
        mx, my = (1, 2) if part == 0 else (2, 1)
        return project(t * 4 + ME, part, at) + from_x[t, mx, :, at].astype(F32) + from_y[t, my, :, at].astype(F32)

    def plane_ready(t):
        ready(t * 4 + ME)
        received(t, 1)
        received(t, 2)

    def z_copy(t, slot, dev):
        return remote(to_z.at[t], from_z.at[slot], szs_sem.at[t], szr_sem.at[slot], dev)

    def z_arrived(slot):
        z_copy(0, slot, pair).wait_recv()

    def z_fill(t, slots):
        def body(at):
            for part in (0, 1):
                v = plane_sum(t, part, at)
                for slot in slots:
                    v = v + from_z[slot, part, :, at].astype(F32)
                to_z[t, part, :, at] = v.astype(BF)

        tiles(body)

    def outer_send(t, slot):
        @pl.when(jnp.logical_not(inner))
        def _():
            z_fill(t, ())
            z_copy(t, slot, pair).start()

    def inner_send(t, add, slot, dev):
        @pl.when(inner)
        def _():
            z_arrived(add)
            z_fill(t, (add,))
            z_copy(t, slot, dev).start()


    listed[...] = jnp.where(mask[...] > 0, ids[...], -1)
    fan = ids.shape[0]
    tall = 128
    next_block = [0]

    def count(blocks):
        first = next_block[0]
        next_block[0] = first + blocks

        def body(i, carry):
            b = i // (rows // tall)
            r = pl.multiple_of(lax.rem(i, rows // tall) * tall, tall)
            base = b * rows + r
            node = lax.broadcasted_iota(jnp.int32, (tall, rows), 0).astype(BF)
            one, zero = jnp.ones((tall, rows), BF), jnp.zeros((tall, rows), BF)
            acc = zero
            for k in range(fan):
                rel = listed[pl.ds(k, 1), :] - base
                rel = jnp.where((rel >= 0) & (rel < tall), rel, -1).astype(F32)
                rel = jnp.broadcast_to(rel, (tall, rows)).astype(BF)
                acc = acc + jnp.where(rel == node, one, zero)
            edges[b, pl.ds(r, tall), :] = acc
            return carry

        lax.fori_loop(first * (rows // tall), (first + blocks) * (rows // tall), body, 0)

    fetch(0)
    w_copy.wait_recv()
    diagonal_out(0)
    raw_out(0)
    fetch(1)
    diagonal_out(1)
    fetch(2)
    fetch(3)
    count(3)
    relay_out(0)
    raw_out(1)
    diagonal_out(2)
    count(5)
    relay_out(1)
    raw_out(2)
    count(4)
    plane_ready(0)
    outer_send(0, 0)
    count(5)
    relay_out(2)
    diagonal_out(3)
    raw_out(3)
    count(2)
    inner_send(0, 0, 2, facing)
    count(3)
    plane_ready(1)
    outer_send(1, 1)
    count(5)
    plane_ready(2)
    outer_send(2, 4)
    inner_send(2, 2, 4, pair)
    inner_send(1, 1, 3, facing)
    count(2)
    relay_out(3)
    count(3)
    plane_ready(3)
    z_arrived(4)

    def last(at):
        hidden[0, :, at] = (plane_sum(3, 0, at) + from_z[4, 0, :, at].astype(F32)).astype(BF)
        self1[:, at] = plane_sum(3, 1, at) + from_z[4, 1, :, at].astype(F32)

    def last_inner(at):
        hidden[0, :, at] = (plane_sum(3, 0, at) + from_z[4, 0, :, at].astype(F32) + from_z[3, 0, :, at].astype(F32)).astype(BF)
        self1[:, at] = plane_sum(3, 1, at) + from_z[4, 1, :, at].astype(F32) + from_z[3, 1, :, at].astype(F32)

    @pl.when(jnp.logical_not(inner))
    def _():
        tiles(last)

    @pl.when(inner)
    def _():
        z_arrived(3)
        tiles(last_inner)

    def finish_scatter():
        w_copy.wait_send()
        for c in mate_copies.values():
            c.wait_send()
        for c in copies.values():
            c.wait_send()
        for t in range(3):
            z_copy(t, 0, pair).wait_send()


    top, bottom = pl.ds(0, half), pl.ds(half, half)

    def average(src, p, after_start):
        started = []

        def go(a, b, send_sem, recv_sem, dev):
            c = remote(a, b, send_sem, recv_sem, dev)
            c.start()
            started.append(c)

        def block(b):
            return full.at[p, b]

        def arrived(dst, recv_sem):
            remote(dst, dst, xs_sem.at[p, 0], recv_sem, mate).wait_recv()

        def add(ref, b, first=False):
            def body(at):
                part = jnp.dot(ref[...], edges[b, :, at], preferred_element_type=F32)
                total[:, at] = part if first else total[:, at] + part

            tiles(body)

        def hop(k, a, b, slot, dev):
            c = remote(a, b, zs_sem.at[p, k], zr_sem.at[p, slot - 1], dev)

            @pl.when(inner)
            def _():
                c.start()

            return c

        go(src, block(me), zs_sem.at[p, 0], zr_sem.at[p, 0], pair)
        hops = [hop(1, src, block(me), 2, facing)]
        go(src, block(me), xs_sem.at[p, 0], xr_sem.at[p, 0], xn)
        go(src, block(me), ys_sem.at[p, 0], yr_sem.at[p, 0], yn)
        go(src, block(me), cs_sem.at[p, 0], cr_sem.at[p, 0], mate)
        after_start()
        add(src, me, True)

        def column(k):
            b = at_plane(me, k)
            arrived(block(b), zr_sem.at[p, k - 1])
            if k == 1:
                hops.append(hop(2, block(b), block(b), 3, facing))
            else:
                hops.append(hop(k + 1, block(b), block(b), k, pair))
            go(block(b), block(b), xs_sem.at[p, k], xr_sem.at[p, k], xn)
            go(block(b), block(b), ys_sem.at[p, k], yr_sem.at[p, k], yn)
            go(block(b), block(b), cs_sem.at[p, k], cr_sem.at[p, k], mate)
            add(block(b), b)

        def relay(k):
            bx, by = at_plane(xn, k), at_plane(yn, k)
            arrived(block(bx), xr_sem.at[p, k])
            go(full.at[p, bx, top], full.at[p, bx, top], ys_sem.at[p, 4 + k], yr_sem.at[p, 4 + k], yn)
            arrived(block(by), yr_sem.at[p, k])
            go(full.at[p, by, bottom], full.at[p, by, bottom], xs_sem.at[p, 4 + k], xr_sem.at[p, 4 + k], xn)
            go(block(bx), block(bx), cs_sem.at[p, 4 + k], cr_sem.at[p, 4 + k], mate)
            go(block(by), block(by), cs_sem.at[p, 8 + k], cr_sem.at[p, 8 + k], mate)
            add(block(bx), bx)
            add(block(by), by)

        def diagonal(k):
            b = at_plane(dg, k)
            arrived(full.at[p, b, top], yr_sem.at[p, 4 + k])
            go(full.at[p, b, top], full.at[p, b, top], cs_sem.at[p, 12 + k], cr_sem.at[p, 12 + k], mate)
            arrived(full.at[p, b, bottom], xr_sem.at[p, 4 + k])
            go(full.at[p, b, bottom], full.at[p, b, bottom], cs_sem.at[p, 16 + k], cr_sem.at[p, 16 + k], mate)
            add(block(b), b)

        def from_mate(k):
            for q, dev in ((0, me), (4, xn), (8, yn)):
                b = at_plane(dev, k) + mate_shift
                arrived(block(b), cr_sem.at[p, q + k])
                add(block(b), b)

        def from_mate_diagonal(k):
            b = at_plane(dg, k) + mate_shift
            arrived(full.at[p, b, top], cr_sem.at[p, 12 + k])
            arrived(full.at[p, b, bottom], cr_sem.at[p, 16 + k])
            add(block(b), b)

        column(1)
        relay(0)
        column(2)
        relay(1)
        column(3)
        from_mate(0)
        diagonal(0)
        relay(2)
        from_mate(1)
        diagonal(1)
        from_mate_diagonal(0)
        relay(3)
        from_mate(2)
        from_mate_diagonal(1)
        diagonal(2)
        from_mate(3)
        from_mate_diagonal(2)
        diagonal(3)
        from_mate_diagonal(3)

        def finish():
            for c in started:
                c.wait_send()

            @pl.when(inner)
            def _():
                for c in hops:
                    c.wait_send()

        return finish

    def mean():
        return total[...] * (1.0 / jnp.sum(mask[...].astype(F32), axis=0, keepdims=True))

    def across_rows(w, v):
        return lax.dot_general(w[...], v, (((0,), (0,)), ((), ())), preferred_element_type=F32)

    finish = average(hidden.at[0], 0, finish_scatter)
    hidden[1] = jnp.maximum(self1[...] + mean(), 0.0).astype(BF)
    finish()
    finish = average(hidden.at[1], 1, lambda: None)
    hidden[2] = jnp.maximum(across_rows(w_self2, hidden[1]) + across_rows(w_nbr2, mean().astype(BF)), 0.0).astype(BF)
    finish()
    finish = average(hidden.at[2], 0, lambda: None)
    out[...] = jnp.dot(w_self3[...], hidden[2], preferred_element_type=F32) + jnp.dot(
        w_nbr3[...], mean().astype(BF), preferred_element_type=F32
    )
    finish()


def solution(mesh):
    def device_step(feat, w_self1, w_nbr1, ids, mask, w_self2, w_nbr2, w_self3, w_nbr3):
        rows, fan = ids.shape
        nodes, depth = feat.shape
        n = nodes // rows
        hid, classes = w_self3.shape
        vmem = pl.BlockSpec(memory_space=pltpu.VMEM)
        dma = pltpu.SemaphoreType.DMA
        logits = pl.pallas_call(
            kernel,
            out_shape=jax.ShapeDtypeStruct((classes, rows), F32),
            in_specs=[pl.BlockSpec(memory_space=pl.ANY)] + [vmem] * 7,
            out_specs=vmem,
            scratch_shapes=[
                pltpu.VMEM((16, depth, rows), BF),
                pltpu.VMEM((16, depth, rows), BF),
                pltpu.VMEM((2 * hid, depth), BF),
                pltpu.VMEM((4, 3, hid, rows), BF),
                pltpu.VMEM((4, 3, hid, rows), BF),
                pltpu.VMEM((4, 3, hid, rows), BF),
                pltpu.VMEM((4, 3, hid, rows), BF),
                pltpu.VMEM((3, 2, hid, rows), BF),
                pltpu.VMEM((5, 2, hid, rows), BF),
                pltpu.VMEM((fan, rows), jnp.int32),
                pltpu.VMEM((n, rows, rows), BF),
                pltpu.VMEM((2, n, hid, rows), BF),
                pltpu.VMEM((hid, rows), F32),
                pltpu.VMEM((hid, rows), F32),
                pltpu.VMEM((3, hid, rows), BF),
                dma((16,)), dma((16,)), dma((16,)), dma((2,)),
                dma((4, 3)), dma((4, 3)), dma((4, 3)), dma((4, 3)), dma((3,)), dma((5,)),
                dma((2, 8)), dma((2, 8)), dma((2, 8)), dma((2, 8)), dma((2, 5)), dma((2, 3)), dma((2, 20)), dma((2, 20)),
            ],
            compiler_params=pltpu.CompilerParams(collective_id=0, has_side_effects=True, vmem_limit_bytes=67043328),
            name="sage",
        )(feat.T, jnp.concatenate([w_nbr1.T, w_self1.T], axis=0), ids.T, mask.T, w_self2, w_nbr2, w_self3.T, w_nbr3.T)
        return logits.T

    col_split, row_split, replicated = P(None, "g"), P("g", None), P()
    return jax.shard_map(
        device_step,
        mesh=mesh,
        in_specs=(col_split, row_split, row_split, row_split, row_split, replicated, replicated, replicated, replicated),
        out_specs=row_split,
        check_vma=False,
    )
```

```python
import jax
import jax.numpy as jnp
from jax import lax
from jax.experimental import pallas as pl
from jax.experimental.pallas import tpu as pltpu
from jax.sharding import PartitionSpec as P

MESH = pl.DeviceIdType.MESH
BF = jnp.bfloat16
F32 = jnp.float32
DG, XN, YN, ME = range(4)


def remote(src, dst, send_sem, recv_sem, dev):
    return pltpu.make_async_remote_copy(
        src_ref=src, dst_ref=dst, send_sem=send_sem, recv_sem=recv_sem, device_id=(dev,), device_id_type=MESH
    )


def kernel(
    feat, w_ref, ids, mask, w_self2, w_nbr2, w_self3, w_nbr3, out,
    own, got, w_got, to_x, to_y, from_x, from_y, to_z, from_z, to_e, from_e, ends_sum, listed, edges, full, total, self1,
    own_sem, gs_sem, gr_sem, w_sem, sxs_sem, sxr_sem, sys_sem, syr_sem, szs_sem, szr_sem, es_sem, er_sem,
    xs_sem, xr_sem, ys_sem, yr_sem, zs_sem, zr_sem, cs_sem, cr_sem,
):
    me = lax.axis_index("g")
    core = lax.rem(me, 2)
    x = lax.rem(me // 2, 2)
    y = lax.rem(me // 4, 2)
    z = me // 8
    spot = y * 2 + x
    mate, xn, yn = me + 1 - 2 * core, me + 2 - 4 * x, me + 4 - 8 * y
    dg = xn + yn - me
    f = (z * (3 - z)) // 2
    inner = f == 1
    across, beyond = 3 - z, z + 2 - 4 * (z // 2)
    planes = (z, z + 1 - 2 * lax.rem(z, 2), f * across + (1 - f) * beyond, f * beyond + (1 - f) * across)

    def at_plane(dev, k):
        return dev + 8 * (planes[k] - z)

    pair = at_plane(me, 1)
    facing = me + 8 * (across - z)
    hid, rows = self1.shape
    tail = 32
    early, late = hid - tail, tail
    main, ends = pl.ds(0, early), pl.ds(early, late)
    chunk = 256

    barrier = pltpu.get_barrier_semaphore()
    for peer in (mate, xn, yn, pair, facing):
        pl.semaphore_signal(barrier, inc=1, device_id=(peer,), device_id_type=MESH)
    pl.semaphore_wait(barrier, 5)

    def tiles(body):
        def step(i, carry):
            body(pl.ds(pl.multiple_of(i * chunk, chunk), chunk))
            return carry

        lax.fori_loop(0, rows // chunk, step, 0)


    w_copy = remote(w_ref, w_got, w_sem.at[0], w_sem.at[1], mate)
    w_copy.start()
    own_copies, mate_copies = {}, {}
    mate_shift = mate - me

    def fetch(t):
        for q, dev in ((DG, dg), (XN, xn), (YN, yn), (ME, me)):
            slot = t * 4 + q
            dest = at_plane(dev, 3 - t)
            a = pltpu.make_async_copy(
                feat.at[:, pl.ds(pl.multiple_of(dest * rows, rows), rows)], own.at[slot], own_sem.at[slot]
            )
            a.start()
            b = remote(
                feat.at[:, pl.ds(pl.multiple_of((dest + mate_shift) * rows, rows), rows)],
                got.at[slot], gs_sem.at[slot], gr_sem.at[slot], mate,
            )
            b.start()
            own_copies[slot], mate_copies[slot] = a, b

    waited = set()

    def ready(slot):
        if slot in waited:
            return
        waited.add(slot)
        own_copies[slot].wait()
        mate_copies[slot].wait_recv()

    def project(slot, part, at, of=None):
        of = pl.ds(part * hid, early if slot < 12 else hid) if of is None else of
        return jnp.dot(w_ref[of, :], own[slot, :, at], preferred_element_type=F32) + jnp.dot(
            w_got[of, :], got[slot, :, at], preferred_element_type=F32
        )

    copies = {}

    def span(t):
        return main if t < 3 else pl.ds(0, hid)

    def keep(ref, t, m, at, v, q, part):
        ref[t, m, main, at] = v[:early].astype(BF)
        if t == 3:
            ref[t, m, ends, at] = (v[early:] + ends_sum[q, pl.ds(part * late, late), at]).astype(BF)

    def send_plane(t, m):
        for name, src, dst, ss, rs, dev in (
            ("x", to_x, from_x, sxs_sem, sxr_sem, xn), ("y", to_y, from_y, sys_sem, syr_sem, yn),
        ):
            c = remote(src.at[t, m, span(t)], dst.at[t, m, span(t)], ss.at[t, m], rs.at[t, m], dev)
            c.start()
            copies[name, t, m] = c

    def received(t, m):
        copies["x", t, m].wait_recv()
        copies["y", t, m].wait_recv()

    def diagonal_out(t):
        ready(t * 4 + DG)

        def body(at):
            keep(to_x, t, 0, at, project(t * 4 + DG, 0, at), DG, 0)
            keep(to_y, t, 0, at, project(t * 4 + DG, 1, at), DG, 1)

        tiles(body)
        send_plane(t, 0)

    def raw_out(t):
        ready(t * 4 + XN)
        ready(t * 4 + YN)

        def body(at):
            keep(to_x, t, 1, at, project(t * 4 + XN, 0, at), XN, 0)
            keep(to_y, t, 1, at, project(t * 4 + YN, 1, at), YN, 1)

        tiles(body)
        send_plane(t, 1)

    def relay_out(t):
        received(t, 0)

        def body(at):
            keep(to_x, t, 2, at, project(t * 4 + XN, 1, at) + from_y[t, 0, span(t), at].astype(F32), XN, 1)
            keep(to_y, t, 2, at, project(t * 4 + YN, 0, at) + from_x[t, 0, span(t), at].astype(F32), YN, 0)

        tiles(body)
        send_plane(t, 2)

    def plane_sum(t, part, at):
        mx, my = (1, 2) if part == 0 else (2, 1)
        return (
            project(t * 4 + ME, part, at)
            + from_x[t, mx, span(t), at].astype(F32)
            + from_y[t, my, span(t), at].astype(F32)
        )

    def plane_ready(t):
        ready(t * 4 + ME)
        received(t, 1)
        received(t, 2)

    def z_copy(t, slot, dev):
        return remote(to_z.at[t], from_z.at[slot], szs_sem.at[t], szr_sem.at[slot], dev)

    def z_arrived(slot):
        z_copy(0, slot, pair).wait_recv()

    def z_fill(t, slots):
        def body(at):
            for part in (0, 1):
                v = plane_sum(t, part, at)
                for slot in slots:
                    v = v + from_z[slot, part, :, at].astype(F32)
                to_z[t, part, :, at] = v.astype(BF)

        tiles(body)

    def outer_send(t, slot):
        @pl.when(jnp.logical_not(inner))
        def _():
            z_fill(t, ())
            z_copy(t, slot, pair).start()

    def inner_send(t, add, slot, dev):
        @pl.when(inner)
        def _():
            z_arrived(add)
            z_fill(t, (add,))
            z_copy(t, slot, dev).start()

    def e_copy(t, slot, dev):
        return remote(to_e.at[t], from_e.at[slot], es_sem.at[t], er_sem.at[slot], dev)

    def e_arrived(slot):
        e_copy(0, slot, pair).wait_recv()

    def e_fill(t, slots):
        for q in range(4):

            def body(at, q=q):
                for part in (0, 1):
                    to = pl.ds(part * late, late)
                    v = project(t * 4 + q, part, at, pl.ds(part * hid + early, late))
                    for slot in slots:
                        v = v + from_e[slot, q, to, at].astype(F32)
                    to_e[t, q, to, at] = v.astype(BF)

            tiles(body)

    def e_outer(t, slot):
        @pl.when(jnp.logical_not(inner))
        def _():
            e_fill(t, ())
            e_copy(t, slot, pair).start()

    def e_inner(t, add, slot, dev):
        @pl.when(inner)
        def _():
            e_arrived(add)
            e_fill(t, (add,))
            e_copy(t, slot, dev).start()

    def e_total():
        e_arrived(4)

        @pl.when(jnp.logical_not(inner))
        def _():
            ends_sum[...] = from_e[4].astype(F32)

        @pl.when(inner)
        def _():
            e_arrived(3)
            ends_sum[...] = from_e[4].astype(F32) + from_e[3].astype(F32)


    listed[...] = jnp.where(mask[...] > 0, ids[...], -1)
    fan = ids.shape[0]
    tall = 128
    next_block = [0]

    def count(blocks):
        first = next_block[0]
        next_block[0] = first + blocks

        def body(i, carry):
            b = i // (rows // tall)
            r = pl.multiple_of(lax.rem(i, rows // tall) * tall, tall)
            base = b * rows + r
            node = lax.broadcasted_iota(jnp.int32, (tall, rows), 0).astype(BF)
            one, zero = jnp.ones((tall, rows), BF), jnp.zeros((tall, rows), BF)
            acc = zero
            for k in range(fan):
                rel = listed[pl.ds(k, 1), :] - base
                rel = jnp.where((rel >= 0) & (rel < tall), rel, -1).astype(F32)
                rel = jnp.broadcast_to(rel, (tall, rows)).astype(BF)
                acc = acc + jnp.where(rel == node, one, zero)
            edges[b, pl.ds(r, tall), :] = acc
            return carry

        lax.fori_loop(first * (rows // tall), (first + blocks) * (rows // tall), body, 0)

    fetch(0)
    w_copy.wait_recv()
    diagonal_out(0)
    raw_out(0)
    fetch(1)
    diagonal_out(1)
    fetch(2)
    fetch(3)
    for slot in (3, 7):
        ready(slot)
    e_outer(0, 0)
    count(3)
    relay_out(0)
    raw_out(1)
    diagonal_out(2)
    e_outer(1, 1)
    for slot in (9, 10, 11):
        ready(slot)
    e_outer(2, 4)
    e_inner(0, 0, 2, facing)
    count(3)
    relay_out(1)
    raw_out(2)
    e_inner(2, 2, 4, pair)
    e_inner(1, 1, 3, facing)
    count(3)
    plane_ready(0)
    outer_send(0, 0)
    count(7)
    e_total()
    relay_out(2)
    diagonal_out(3)
    raw_out(3)
    count(3)
    inner_send(0, 0, 2, facing)
    count(3)
    plane_ready(1)
    outer_send(1, 1)
    count(5)
    plane_ready(2)
    outer_send(2, 4)
    inner_send(2, 2, 4, pair)
    inner_send(1, 1, 3, facing)
    count(2)
    relay_out(3)
    count(3)
    assert next_block[0] == edges.shape[0]
    plane_ready(3)
    z_arrived(4)

    mine = (z, core, spot)

    def last(part, slots, out_ref):
        def body(at):
            v = plane_sum(3, part, at)
            w = v[:early]
            for slot in slots:
                w = w + from_z[slot, part, :, at].astype(F32)
            out_ref[main, at] = w.astype(out_ref.dtype)
            out_ref[ends, at] = (v[early:] + ends_sum[ME, pl.ds(part * late, late), at]).astype(out_ref.dtype)

        tiles(body)

    @pl.when(jnp.logical_not(inner))
    def _():
        last(0, (4,), full.at[0, z, core, spot])

    @pl.when(inner)
    def _():
        z_arrived(3)
        last(0, (4, 3), full.at[0, z, core, spot])

    def finish_scatter():
        @pl.when(jnp.logical_not(inner))
        def _():
            last(1, (4,), self1)

        @pl.when(inner)
        def _():
            last(1, (4, 3), self1)

        w_copy.wait_send()
        for c in mate_copies.values():
            c.wait_send()
        for c in copies.values():
            c.wait_send()
        for t in range(3):
            z_copy(t, 0, pair).wait_send()
            e_copy(t, 0, pair).wait_send()


    top, bottom = pl.ds(0, early // 2), pl.ds(early // 2, early // 2)
    ends_top, ends_bottom = pl.ds(early, late // 2), pl.ds(early + late // 2, late // 2)
    spot_x, spot_y = y * 2 + 1 - x, (1 - y) * 2 + x
    spot_d = 3 - spot

    def average(p, after_start):
        started = []

        def go(ref, send_sem, recv_sem, dev):
            c = remote(ref, ref, send_sem, recv_sem, dev)
            c.start()
            started.append(c)

        def piece(k, q, part, c=core):
            return full.at[p, planes[k], c, q, part]

        def arrived(dst, recv_sem):
            remote(dst, dst, xs_sem.at[p, 0], recv_sem, mate).wait_recv()

        def add(k, q, c=core, first=False):
            ref = full.at[p, planes[k], c, q]
            b = planes[k] * 8 + q * 2 + c

            def body(at):
                part = jnp.dot(ref[...], edges[b, :, at], preferred_element_type=F32)
                total[:, at] = part if first else total[:, at] + part

            tiles(body)

        hops = []

        def hop(ref, send, slot, dev):
            c = remote(ref, ref, zs_sem.at[p, send], zr_sem.at[p, slot], dev)

            @pl.when(inner)
            def _():
                c.start()

            hops.append(c)

        def to_plane(ref_x, ref_y, n):
            go(ref_x, xs_sem.at[p, n], xr_sem.at[p, n], xn)
            go(ref_y, ys_sem.at[p, n], yr_sem.at[p, n], yn)

        def to_mate(ref, n):
            go(ref, cs_sem.at[p, n], cr_sem.at[p, n], mate)

        def all_ends(k, c=core):
            return full.at[p, planes[k], c, :, ends]

        go(piece(0, spot, main), zs_sem.at[p, 0], zr_sem.at[p, 0], pair)
        hop(piece(0, spot, main), 1, 1, facing)
        to_plane(piece(0, spot, ends), piece(0, spot, ends), 8)
        to_plane(piece(0, spot, top), piece(0, spot, bottom), 0)
        to_mate(full.at[p, z, core, spot], 0)
        arrived(piece(0, spot_x, ends), xr_sem.at[p, 8])
        arrived(piece(0, spot_y, ends), yr_sem.at[p, 8])
        to_plane(piece(0, spot_y, ends_bottom), piece(0, spot_x, ends_top), 9)
        to_plane(piece(0, spot, bottom), piece(0, spot, top), 10)
        to_mate(piece(0, spot_x, ends), 20)
        to_mate(piece(0, spot_y, ends), 21)
        after_start()
        add(0, spot, first=True)

        def column(k):
            ref = piece(k, spot, main)
            arrived(ref, zr_sem.at[p, k - 1])
            if k == 1:
                hop(ref, 2, 2, facing)
            else:
                hop(ref, k + 1, k - 1, pair)
            to_plane(ref, ref, k)
            to_mate(ref, k)

        def own_ends():
            arrived(piece(0, spot_d, ends_top), yr_sem.at[p, 9])
            arrived(piece(0, spot_d, ends_bottom), xr_sem.at[p, 9])
            go(all_ends(0), zs_sem.at[p, 5], zr_sem.at[p, 3], pair)
            hop(all_ends(0), 6, 4, facing)
            to_mate(piece(0, spot_d, ends), 22)

        def ends_of(k):
            ref = all_ends(k)
            arrived(ref, zr_sem.at[p, 2 + k])
            if k == 1:
                hop(ref, 7, 5, facing)
            else:
                hop(ref, 6 + k, 2 + k, pair)
            to_mate(ref, 23 + k)
            add(k, spot)

        def relay(k):
            if k == 0:
                arrived(piece(0, spot_x, top), xr_sem.at[p, 0])
                arrived(piece(0, spot_y, bottom), yr_sem.at[p, 0])
                to_plane(piece(0, spot_y, bottom), piece(0, spot_x, top), 4)
                arrived(piece(0, spot_x, bottom), xr_sem.at[p, 10])
                arrived(piece(0, spot_y, top), yr_sem.at[p, 10])
            else:
                arrived(piece(k, spot_x, main), xr_sem.at[p, k])
                arrived(piece(k, spot_y, main), yr_sem.at[p, k])
                to_plane(piece(k, spot_y, bottom), piece(k, spot_x, top), 4 + k)
            to_mate(piece(k, spot_x, main), 4 + k)
            to_mate(piece(k, spot_y, main), 8 + k)
            add(k, spot_x)
            add(k, spot_y)

        def diagonal(k):
            arrived(piece(k, spot_d, top), yr_sem.at[p, 4 + k])
            to_mate(piece(k, spot_d, top), 12 + k)
            arrived(piece(k, spot_d, bottom), xr_sem.at[p, 4 + k])
            to_mate(piece(k, spot_d, bottom), 16 + k)
            add(k, spot_d)

        other = 1 - core

        def from_mate(k):
            if k == 0:
                arrived(full.at[p, z, other, spot], cr_sem.at[p, 0])
                arrived(piece(0, spot_x, ends, other), cr_sem.at[p, 20])
                arrived(piece(0, spot_y, ends, other), cr_sem.at[p, 21])
            else:
                arrived(all_ends(k, other), cr_sem.at[p, 23 + k])
                arrived(piece(k, spot, main, other), cr_sem.at[p, k])
            add(k, spot, other)
            arrived(piece(k, spot_x, main, other), cr_sem.at[p, 4 + k])
            add(k, spot_x, other)
            arrived(piece(k, spot_y, main, other), cr_sem.at[p, 8 + k])
            add(k, spot_y, other)

        def from_mate_diagonal(k):
            if k == 0:
                arrived(piece(0, spot_d, ends, other), cr_sem.at[p, 22])
            arrived(piece(k, spot_d, top, other), cr_sem.at[p, 12 + k])
            arrived(piece(k, spot_d, bottom, other), cr_sem.at[p, 16 + k])
            add(k, spot_d, other)

        own_ends()
        column(1)
        relay(0)
        column(2)
        ends_of(1)
        relay(1)
        column(3)
        from_mate(0)
        diagonal(0)
        ends_of(2)
        relay(2)
        from_mate(1)
        diagonal(1)
        from_mate_diagonal(0)
        ends_of(3)
        relay(3)
        from_mate(2)
        from_mate_diagonal(1)
        diagonal(2)
        from_mate(3)
        from_mate_diagonal(2)
        diagonal(3)
        from_mate_diagonal(3)

        def finish():
            for c in started:
                c.wait_send()

            @pl.when(inner)
            def _():
                for c in hops:
                    c.wait_send()

        return finish

    def mean():
        return total[...] * (1.0 / jnp.sum(mask[...].astype(F32), axis=0, keepdims=True))

    def across_rows(w, v):
        return lax.dot_general(w[...], v, (((0,), (0,)), ((), ())), preferred_element_type=F32)

    def put(p, v):
        full[(p,) + mine] = jnp.maximum(v, 0.0).astype(BF)

    def self_two():
        self1[...] = across_rows(w_self2, full[(1,) + mine])

    def self_three():
        out[...] = jnp.dot(w_self3[...], full[(0,) + mine], preferred_element_type=F32)

    finish = average(0, finish_scatter)
    put(1, self1[...] + mean())
    finish()
    finish = average(1, self_two)
    put(0, self1[...] + across_rows(w_nbr2, mean().astype(BF)))
    finish()
    finish = average(0, self_three)
    out[...] += jnp.dot(w_nbr3[...], mean().astype(BF), preferred_element_type=F32)
    finish()


def solution(mesh):
    def device_step(feat, w_self1, w_nbr1, ids, mask, w_self2, w_nbr2, w_self3, w_nbr3):
        rows, fan = ids.shape
        nodes, depth = feat.shape
        n = nodes // rows
        hid, classes = w_self3.shape
        vmem = pl.BlockSpec(memory_space=pltpu.VMEM)
        dma = pltpu.SemaphoreType.DMA
        logits = pl.pallas_call(
            kernel,
            out_shape=jax.ShapeDtypeStruct((classes, rows), F32),
            in_specs=[pl.BlockSpec(memory_space=pl.ANY)] + [vmem] * 7,
            out_specs=vmem,
            scratch_shapes=[
                pltpu.VMEM((16, depth, rows), BF),
                pltpu.VMEM((16, depth, rows), BF),
                pltpu.VMEM((2 * hid, depth), BF),
                pltpu.VMEM((4, 3, hid, rows), BF),
                pltpu.VMEM((4, 3, hid, rows), BF),
                pltpu.VMEM((4, 3, hid, rows), BF),
                pltpu.VMEM((4, 3, hid, rows), BF),
                pltpu.VMEM((3, 2, hid - 32, rows), BF),
                pltpu.VMEM((5, 2, hid - 32, rows), BF),
                pltpu.VMEM((3, 4, 64, rows), BF),
                pltpu.VMEM((5, 4, 64, rows), BF),
                pltpu.VMEM((4, 64, rows), F32),
                pltpu.VMEM((fan, rows), jnp.int32),
                pltpu.VMEM((n, rows, rows), BF),
                pltpu.VMEM((2, 4, 2, 4, hid, rows), BF),
                pltpu.VMEM((hid, rows), F32),
                pltpu.VMEM((hid, rows), F32),
                dma((16,)), dma((16,)), dma((16,)), dma((2,)),
                dma((4, 3)), dma((4, 3)), dma((4, 3)), dma((4, 3)), dma((3,)), dma((5,)), dma((3,)), dma((5,)),
                dma((2, 11)), dma((2, 11)), dma((2, 11)), dma((2, 11)), dma((2, 10)), dma((2, 6)), dma((2, 27)), dma((2, 27)),
            ],
            compiler_params=pltpu.CompilerParams(collective_id=0, has_side_effects=True, vmem_limit_bytes=67043328),
            name="sage",
        )(feat.T, jnp.concatenate([w_nbr1.T, w_self1.T], axis=0), ids.T, mask.T, w_self2, w_nbr2, w_self3.T, w_nbr3.T)
        return logits.T

    col_split, row_split, replicated = P(None, "g"), P("g", None), P()
    return jax.shard_map(
        device_step,
        mesh=mesh,
        in_specs=(col_split, row_split, row_split, row_split, row_split, replicated, replicated, replicated, replicated),
        out_specs=row_split,
        check_vma=False,
    )
```

```python
import jax
import jax.numpy as jnp
from jax import lax
from jax.experimental import pallas as pl
from jax.experimental.pallas import tpu as pltpu
from jax.sharding import PartitionSpec as P

MESH = pl.DeviceIdType.MESH
BF = jnp.bfloat16
F32 = jnp.float32
DG, XN, YN, ME = range(4)


def remote(src, dst, send_sem, recv_sem, dev):
    return pltpu.make_async_remote_copy(
        src_ref=src, dst_ref=dst, send_sem=send_sem, recv_sem=recv_sem, device_id=(dev,), device_id_type=MESH
    )


def kernel(
    feat, w_nbr1, w_self1, ids, mask, w_self2, w_nbr2, w_self3, w_nbr3, out,
    own, got, w_ref, w_got, to_x, to_y, from_x, from_y, to_z, from_z, to_e, from_e, ends_sum, listed, edges, full, total, self1,
    own_sem, gs_sem, gr_sem, w_sem, sxs_sem, sxr_sem, sys_sem, syr_sem, szs_sem, szr_sem, es_sem, er_sem,
    xs_sem, xr_sem, ys_sem, yr_sem, zs_sem, zr_sem, cs_sem, cr_sem,
):
    me = lax.axis_index("g")
    core = lax.rem(me, 2)
    x = lax.rem(me // 2, 2)
    y = lax.rem(me // 4, 2)
    z = me // 8
    spot = y * 2 + x
    mate, xn, yn = me + 1 - 2 * core, me + 2 - 4 * x, me + 4 - 8 * y
    dg = xn + yn - me
    f = (z * (3 - z)) // 2
    inner = f == 1
    across, beyond = 3 - z, z + 2 - 4 * (z // 2)
    planes = (z, z + 1 - 2 * lax.rem(z, 2), f * across + (1 - f) * beyond, f * beyond + (1 - f) * across)

    def at_plane(dev, k):
        return dev + 8 * (planes[k] - z)

    pair = at_plane(me, 1)
    facing = me + 8 * (across - z)
    hid, rows = self1.shape
    tail = 32
    early, late = hid - tail, tail
    main, ends = pl.ds(0, early), pl.ds(early, late)
    chunk = 256

    barrier = pltpu.get_barrier_semaphore()
    for peer in (mate, xn, yn, pair, facing):
        pl.semaphore_signal(barrier, inc=1, device_id=(peer,), device_id_type=MESH)
    pl.semaphore_wait(barrier, 5)

    def tiles(body):
        def step(i, carry):
            body(pl.ds(pl.multiple_of(i * chunk, chunk), chunk))
            return carry

        lax.fori_loop(0, rows // chunk, step, 0)


    for part, w in ((0, w_nbr1), (1, w_self1)):
        w_ref[pl.ds(part * hid, hid), :] = jnp.transpose(w[...].astype(F32)).astype(BF)
    w_copy = remote(w_ref, w_got, w_sem.at[0], w_sem.at[1], mate)
    w_copy.start()
    own_copies, mate_copies = {}, {}
    mate_shift = mate - me

    def fetch(t):
        for q, dev in ((DG, dg), (XN, xn), (YN, yn), (ME, me)):
            slot = t * 4 + q
            dest = at_plane(dev, 3 - t)
            a = pltpu.make_async_copy(
                feat.at[:, pl.ds(pl.multiple_of(dest * rows, rows), rows)], own.at[slot], own_sem.at[slot]
            )
            a.start()
            b = remote(
                feat.at[:, pl.ds(pl.multiple_of((dest + mate_shift) * rows, rows), rows)],
                got.at[slot], gs_sem.at[slot], gr_sem.at[slot], mate,
            )
            b.start()
            own_copies[slot], mate_copies[slot] = a, b

    waited = set()

    def ready(slot):
        if slot in waited:
            return
        waited.add(slot)
        own_copies[slot].wait()
        mate_copies[slot].wait_recv()

    def project(slot, part, at, of=None):
        of = pl.ds(part * hid, early if slot < 12 else hid) if of is None else of
        return jnp.dot(w_ref[of, :], own[slot, :, at], preferred_element_type=F32) + jnp.dot(
            w_got[of, :], got[slot, :, at], preferred_element_type=F32
        )

    copies = {}

    def span(t):
        return main if t < 3 else pl.ds(0, hid)

    def keep(ref, t, m, at, v, q, part):
        ref[t, m, main, at] = v[:early].astype(BF)
        if t == 3:
            ref[t, m, ends, at] = (v[early:] + ends_sum[q, pl.ds(part * late, late), at]).astype(BF)

    def send_plane(t, m):
        for name, src, dst, ss, rs, dev in (
            ("x", to_x, from_x, sxs_sem, sxr_sem, xn), ("y", to_y, from_y, sys_sem, syr_sem, yn),
        ):
            c = remote(src.at[t, m, span(t)], dst.at[t, m, span(t)], ss.at[t, m], rs.at[t, m], dev)
            c.start()
            copies[name, t, m] = c

    def received(t, m):
        copies["x", t, m].wait_recv()
        copies["y", t, m].wait_recv()

    def diagonal_out(t):
        ready(t * 4 + DG)

        def body(at):
            keep(to_x, t, 0, at, project(t * 4 + DG, 0, at), DG, 0)
            keep(to_y, t, 0, at, project(t * 4 + DG, 1, at), DG, 1)

        tiles(body)
        send_plane(t, 0)

    def raw_out(t):
        ready(t * 4 + XN)
        ready(t * 4 + YN)

        def body(at):
            keep(to_x, t, 1, at, project(t * 4 + XN, 0, at), XN, 0)
            keep(to_y, t, 1, at, project(t * 4 + YN, 1, at), YN, 1)

        tiles(body)
        send_plane(t, 1)

    def relay_out(t):
        received(t, 0)

        def body(at):
            keep(to_x, t, 2, at, project(t * 4 + XN, 1, at) + from_y[t, 0, span(t), at].astype(F32), XN, 1)
            keep(to_y, t, 2, at, project(t * 4 + YN, 0, at) + from_x[t, 0, span(t), at].astype(F32), YN, 0)

        tiles(body)
        send_plane(t, 2)

    def plane_sum(t, part, at):
        mx, my = (1, 2) if part == 0 else (2, 1)
        return (
            project(t * 4 + ME, part, at)
            + from_x[t, mx, span(t), at].astype(F32)
            + from_y[t, my, span(t), at].astype(F32)
        )

    def plane_ready(t):
        ready(t * 4 + ME)
        received(t, 1)
        received(t, 2)

    def z_copy(t, slot, dev):
        return remote(to_z.at[t], from_z.at[slot], szs_sem.at[t], szr_sem.at[slot], dev)

    def z_arrived(slot):
        z_copy(0, slot, pair).wait_recv()

    def z_fill(t, slots):
        def body(at):
            for part in (0, 1):
                v = plane_sum(t, part, at)
                for slot in slots:
                    v = v + from_z[slot, part, :, at].astype(F32)
                to_z[t, part, :, at] = v.astype(BF)

        tiles(body)

    def outer_send(t, slot):
        @pl.when(jnp.logical_not(inner))
        def _():
            z_fill(t, ())
            z_copy(t, slot, pair).start()

    def inner_send(t, add, slot, dev):
        @pl.when(inner)
        def _():
            z_arrived(add)
            z_fill(t, (add,))
            z_copy(t, slot, dev).start()

    def e_copy(t, slot, dev):
        return remote(to_e.at[t], from_e.at[slot], es_sem.at[t], er_sem.at[slot], dev)

    def e_arrived(slot):
        e_copy(0, slot, pair).wait_recv()

    def e_fill(t, slots):
        for q in range(4):

            def body(at, q=q):
                for part in (0, 1):
                    to = pl.ds(part * late, late)
                    v = project(t * 4 + q, part, at, pl.ds(part * hid + early, late))
                    for slot in slots:
                        v = v + from_e[slot, q, to, at].astype(F32)
                    to_e[t, q, to, at] = v.astype(BF)

            tiles(body)

    def e_outer(t, slot):
        @pl.when(jnp.logical_not(inner))
        def _():
            e_fill(t, ())
            e_copy(t, slot, pair).start()

    def e_inner(t, add, slot, dev):
        @pl.when(inner)
        def _():
            e_arrived(add)
            e_fill(t, (add,))
            e_copy(t, slot, dev).start()

    def e_total():
        e_arrived(4)

        @pl.when(jnp.logical_not(inner))
        def _():
            ends_sum[...] = from_e[4].astype(F32)

        @pl.when(inner)
        def _():
            e_arrived(3)
            ends_sum[...] = from_e[4].astype(F32) + from_e[3].astype(F32)


    listed[...] = jnp.where(mask[...] > 0, ids[...], -1)
    fan = ids.shape[0]
    tall = 128
    next_block = [0]

    def count(blocks):
        first = next_block[0]
        next_block[0] = first + blocks

        def body(i, carry):
            b = i // (rows // tall)
            r = pl.multiple_of(lax.rem(i, rows // tall) * tall, tall)
            base = b * rows + r
            node = lax.broadcasted_iota(jnp.int32, (tall, rows), 0).astype(BF)
            one, zero = jnp.ones((tall, rows), BF), jnp.zeros((tall, rows), BF)
            acc = zero
            for k in range(fan):
                rel = listed[pl.ds(k, 1), :] - base
                rel = jnp.where((rel >= 0) & (rel < tall), rel, -1).astype(F32)
                rel = jnp.broadcast_to(rel, (tall, rows)).astype(BF)
                acc = acc + jnp.where(rel == node, one, zero)
            edges[b, pl.ds(r, tall), :] = acc
            return carry

        lax.fori_loop(first * (rows // tall), (first + blocks) * (rows // tall), body, 0)

    fetch(0)
    w_copy.wait_recv()
    diagonal_out(0)
    raw_out(0)
    fetch(1)
    diagonal_out(1)
    fetch(2)
    fetch(3)
    for slot in (3, 7):
        ready(slot)
    e_outer(0, 0)
    count(3)
    relay_out(0)
    raw_out(1)
    diagonal_out(2)
    e_outer(1, 1)
    for slot in (9, 10, 11):
        ready(slot)
    e_outer(2, 4)
    e_inner(0, 0, 2, facing)
    count(3)
    relay_out(1)
    raw_out(2)
    e_inner(2, 2, 4, pair)
    e_inner(1, 1, 3, facing)
    count(3)
    plane_ready(0)
    outer_send(0, 0)
    count(7)
    e_total()
    relay_out(2)
    diagonal_out(3)
    raw_out(3)
    count(3)
    inner_send(0, 0, 2, facing)
    count(3)
    plane_ready(1)
    outer_send(1, 1)
    count(5)
    plane_ready(2)
    outer_send(2, 4)
    inner_send(2, 2, 4, pair)
    inner_send(1, 1, 3, facing)
    count(2)
    relay_out(3)
    count(3)
    assert next_block[0] == edges.shape[0]
    plane_ready(3)
    z_arrived(4)

    mine = (z, core, spot)

    def last(part, slots, out_ref):
        def body(at):
            v = plane_sum(3, part, at)
            w = v[:early]
            for slot in slots:
                w = w + from_z[slot, part, :, at].astype(F32)
            out_ref[main, at] = w.astype(out_ref.dtype)
            out_ref[ends, at] = (v[early:] + ends_sum[ME, pl.ds(part * late, late), at]).astype(out_ref.dtype)

        tiles(body)

    @pl.when(jnp.logical_not(inner))
    def _():
        last(0, (4,), full.at[0, z, core, spot])

    @pl.when(inner)
    def _():
        z_arrived(3)
        last(0, (4, 3), full.at[0, z, core, spot])

    def finish_scatter():
        @pl.when(jnp.logical_not(inner))
        def _():
            last(1, (4,), self1)

        @pl.when(inner)
        def _():
            last(1, (4, 3), self1)

        w_copy.wait_send()
        for c in mate_copies.values():
            c.wait_send()
        for c in copies.values():
            c.wait_send()
        for t in range(3):
            z_copy(t, 0, pair).wait_send()
            e_copy(t, 0, pair).wait_send()


    top, bottom = pl.ds(0, early // 2), pl.ds(early // 2, early // 2)
    ends_top, ends_bottom = pl.ds(early, late // 2), pl.ds(early + late // 2, late // 2)
    spot_x, spot_y = y * 2 + 1 - x, (1 - y) * 2 + x
    spot_d = 3 - spot

    def average(p, after_start):
        started = []

        def go(ref, send_sem, recv_sem, dev):
            c = remote(ref, ref, send_sem, recv_sem, dev)
            c.start()
            started.append(c)

        def piece(k, q, part, c=core):
            return full.at[p, planes[k], c, q, part]

        def arrived(dst, recv_sem):
            remote(dst, dst, xs_sem.at[p, 0], recv_sem, mate).wait_recv()

        def add(k, *places, c=core, first=False):
            def body(at):
                part = None if first else total[:, at]
                for q in places:
                    b = planes[k] * 8 + q * 2 + c
                    term = jnp.dot(full[p, planes[k], c, q], edges[b, :, at], preferred_element_type=F32)
                    part = term if part is None else part + term
                total[:, at] = part

            tiles(body)

        hops = []

        def hop(ref, send, slot, dev):
            c = remote(ref, ref, zs_sem.at[p, send], zr_sem.at[p, slot], dev)

            @pl.when(inner)
            def _():
                c.start()

            hops.append(c)

        def to_plane(ref_x, ref_y, n):
            go(ref_x, xs_sem.at[p, n], xr_sem.at[p, n], xn)
            go(ref_y, ys_sem.at[p, n], yr_sem.at[p, n], yn)

        def to_mate(ref, n):
            go(ref, cs_sem.at[p, n], cr_sem.at[p, n], mate)

        def all_ends(k, c=core):
            return full.at[p, planes[k], c, :, ends]

        go(piece(0, spot, main), zs_sem.at[p, 0], zr_sem.at[p, 0], pair)
        hop(piece(0, spot, main), 1, 1, facing)
        to_plane(piece(0, spot, ends), piece(0, spot, ends), 8)
        to_plane(piece(0, spot, top), piece(0, spot, bottom), 0)
        to_mate(full.at[p, z, core, spot], 0)
        arrived(piece(0, spot_x, ends), xr_sem.at[p, 8])
        arrived(piece(0, spot_y, ends), yr_sem.at[p, 8])
        to_plane(piece(0, spot_y, ends_bottom), piece(0, spot_x, ends_top), 9)
        to_plane(piece(0, spot, bottom), piece(0, spot, top), 10)
        to_mate(piece(0, spot_x, ends), 20)
        to_mate(piece(0, spot_y, ends), 21)
        after_start()
        add(0, spot, first=True)

        def column(k):
            ref = piece(k, spot, main)
            arrived(ref, zr_sem.at[p, k - 1])
            if k == 1:
                hop(ref, 2, 2, facing)
            else:
                hop(ref, k + 1, k - 1, pair)
            to_plane(ref, ref, k)
            to_mate(ref, k)

        def own_ends():
            arrived(piece(0, spot_d, ends_top), yr_sem.at[p, 9])
            arrived(piece(0, spot_d, ends_bottom), xr_sem.at[p, 9])
            go(all_ends(0), zs_sem.at[p, 5], zr_sem.at[p, 3], pair)
            hop(all_ends(0), 6, 4, facing)
            to_mate(piece(0, spot_d, ends), 22)

        def ends_of(k):
            ref = all_ends(k)
            arrived(ref, zr_sem.at[p, 2 + k])
            if k == 1:
                hop(ref, 7, 5, facing)
            else:
                hop(ref, 6 + k, 2 + k, pair)
            to_mate(ref, 23 + k)

        def relay(k):
            if k == 0:
                arrived(piece(0, spot_x, top), xr_sem.at[p, 0])
                arrived(piece(0, spot_y, bottom), yr_sem.at[p, 0])
                to_plane(piece(0, spot_y, bottom), piece(0, spot_x, top), 4)
                arrived(piece(0, spot_x, bottom), xr_sem.at[p, 10])
                arrived(piece(0, spot_y, top), yr_sem.at[p, 10])
            else:
                arrived(piece(k, spot_x, main), xr_sem.at[p, k])
                arrived(piece(k, spot_y, main), yr_sem.at[p, k])
                to_plane(piece(k, spot_y, bottom), piece(k, spot_x, top), 4 + k)
            to_mate(piece(k, spot_x, main), 4 + k)
            to_mate(piece(k, spot_y, main), 8 + k)

        def diagonal(k):
            arrived(piece(k, spot_d, top), yr_sem.at[p, 4 + k])
            to_mate(piece(k, spot_d, top), 12 + k)
            arrived(piece(k, spot_d, bottom), xr_sem.at[p, 4 + k])
            to_mate(piece(k, spot_d, bottom), 16 + k)
            add(k, spot_d)

        other = 1 - core

        def from_mate(k):
            if k == 0:
                arrived(full.at[p, z, other, spot], cr_sem.at[p, 0])
                arrived(piece(0, spot_x, ends, other), cr_sem.at[p, 20])
                arrived(piece(0, spot_y, ends, other), cr_sem.at[p, 21])
            else:
                arrived(all_ends(k, other), cr_sem.at[p, 23 + k])
                arrived(piece(k, spot, main, other), cr_sem.at[p, k])
            arrived(piece(k, spot_x, main, other), cr_sem.at[p, 4 + k])
            arrived(piece(k, spot_y, main, other), cr_sem.at[p, 8 + k])
            add(k, spot, spot_x, spot_y, c=other)

        def from_mate_diagonal(k):
            if k == 0:
                arrived(piece(0, spot_d, ends, other), cr_sem.at[p, 22])
            arrived(piece(k, spot_d, top, other), cr_sem.at[p, 12 + k])
            arrived(piece(k, spot_d, bottom, other), cr_sem.at[p, 16 + k])
            add(k, spot_d, c=other)

        own_ends()
        column(1)
        relay(0)
        add(0, spot_x, spot_y)
        column(2)
        ends_of(1)
        relay(1)
        add(1, spot, spot_x, spot_y)
        column(3)
        ends_of(2)
        from_mate(0)
        diagonal(0)
        relay(2)
        add(2, spot, spot_x, spot_y)
        ends_of(3)
        from_mate(1)
        diagonal(1)
        from_mate_diagonal(0)
        from_mate(2)
        relay(3)
        add(3, spot, spot_x, spot_y)
        from_mate_diagonal(1)
        diagonal(2)
        from_mate(3)
        from_mate_diagonal(2)
        diagonal(3)
        from_mate_diagonal(3)

        def finish():
            for c in started:
                c.wait_send()

            @pl.when(inner)
            def _():
                for c in hops:
                    c.wait_send()

        return finish

    def mean():
        return total[...] * (1.0 / jnp.sum(mask[...].astype(F32), axis=0, keepdims=True))

    def across_rows(w, v):
        return lax.dot_general(w[...], v, (((0,), (0,)), ((), ())), preferred_element_type=F32)

    def put(p, v):
        full[(p,) + mine] = jnp.maximum(v, 0.0).astype(BF)

    def self_two():
        self1[...] = across_rows(w_self2, full[(1,) + mine])

    def self_three():
        out[...] = jnp.dot(w_self3[...], full[(0,) + mine], preferred_element_type=F32)

    finish = average(0, finish_scatter)
    put(1, self1[...] + mean())
    finish()
    finish = average(1, self_two)
    put(0, self1[...] + across_rows(w_nbr2, mean().astype(BF)))
    finish()
    finish = average(0, self_three)
    out[...] += jnp.dot(w_nbr3[...], mean().astype(BF), preferred_element_type=F32)
    finish()


def solution(mesh):
    def device_step(feat, w_self1, w_nbr1, ids, mask, w_self2, w_nbr2, w_self3, w_nbr3):
        rows, fan = ids.shape
        nodes, depth = feat.shape
        n = nodes // rows
        hid, classes = w_self3.shape
        vmem = pl.BlockSpec(memory_space=pltpu.VMEM)
        dma = pltpu.SemaphoreType.DMA
        logits = pl.pallas_call(
            kernel,
            out_shape=jax.ShapeDtypeStruct((classes, rows), F32),
            in_specs=[pl.BlockSpec(memory_space=pl.ANY)] + [vmem] * 8,
            out_specs=vmem,
            scratch_shapes=[
                pltpu.VMEM((16, depth, rows), BF),
                pltpu.VMEM((16, depth, rows), BF),
                pltpu.VMEM((2 * hid, depth), BF),
                pltpu.VMEM((2 * hid, depth), BF),
                pltpu.VMEM((4, 3, hid, rows), BF),
                pltpu.VMEM((4, 3, hid, rows), BF),
                pltpu.VMEM((4, 3, hid, rows), BF),
                pltpu.VMEM((4, 3, hid, rows), BF),
                pltpu.VMEM((3, 2, hid - 32, rows), BF),
                pltpu.VMEM((5, 2, hid - 32, rows), BF),
                pltpu.VMEM((3, 4, 64, rows), BF),
                pltpu.VMEM((5, 4, 64, rows), BF),
                pltpu.VMEM((4, 64, rows), F32),
                pltpu.VMEM((fan, rows), jnp.int32),
                pltpu.VMEM((n, rows, rows), BF),
                pltpu.VMEM((2, 4, 2, 4, hid, rows), BF),
                pltpu.VMEM((hid, rows), F32),
                pltpu.VMEM((hid, rows), F32),
                dma((16,)), dma((16,)), dma((16,)), dma((2,)),
                dma((4, 3)), dma((4, 3)), dma((4, 3)), dma((4, 3)), dma((3,)), dma((5,)), dma((3,)), dma((5,)),
                dma((2, 11)), dma((2, 11)), dma((2, 11)), dma((2, 11)), dma((2, 10)), dma((2, 6)), dma((2, 27)), dma((2, 27)),
            ],
            compiler_params=pltpu.CompilerParams(collective_id=0, has_side_effects=True, vmem_limit_bytes=67043328),
            name="sage",
        )(feat.T, w_nbr1, w_self1, ids.T, mask.T, w_self2, w_nbr2, w_self3.T, w_nbr3.T)
        return logits.T

    col_split, row_split, replicated = P(None, "g"), P("g", None), P()
    return jax.shard_map(
        device_step,
        mesh=mesh,
        in_specs=(col_split, row_split, row_split, row_split, row_split, replicated, replicated, replicated, replicated),
        out_specs=row_split,
        check_vma=False,
    )
```
